32 devices in a mesh: scen: 2 (over x), lon: 16 (over z, y, core).
Axes of the slice: x: 2, y: 2, z: 4, core: 2. Of those that a mesh axis runs over, the one named last changes fastest.
Arguments:
- tracer: float32 [16, 4, 512, 1024], P('scen', None, 'lon'), parts along dimension 0, may hold values from 0.25 to 15, as said below
- offsets: int32 [4, 512, 1024], P(None, 'lon'), may hold values from -12 to 12
- frac: float32 [4, 1024], replicated, may hold values from 0.02 to 0.98
- air_before: float32 [4, 512, 1024], P(None, 'lon'), may hold values from 0.5 to 2
- air_after: float32 [4, 512, 1024], P(None, 'lon'), may hold values from 0.05 to 15, as said below
- growth: float32 [16], P('scen'), parts along dimension 0, may hold values from 0.05 to 0.5
Outputs:
- tracer_next: float32 [16, 4, 512, 1024], P('scen', None, 'lon'), parts along dimension 0
The draws below stay inside these ranges and needn't reach their ends.
There are 2 independent parts, one for each index of `scen`. The reference program is written for one: setup_inputs(seed, part) draws one part's arguments, and reference() takes and returns one part's arrays. A program takes and returns all parts, laid end to end along the dimension named above; an argument that names none is the same for every part. Nothing has to cross between parts.
Inputs may be any that keep to these rules, and one draw needn't show every extreme that they name: `tracer`: positive mixing ratios. `air_after`: positive air masses.
All inputs are finite; a program needn't handle non-finite values.
Results may differ from the reference program's by a relative error of at most 0.00002.
Values sent between devices are 32-bit elements; how exact they have to be, the bound alone decides.
A program may use at most 64 MiB of HBM per device.

```python
import math
import jax
import jax.numpy as jnp
from jax import lax

S = 8
LEV = 4
NLAT = 1024
OFFMAX = 12
NLON = 512


def draw_tracer(key, part):
    shape = (S, LEV, NLON, NLAT)
    column = jnp.arange(NLON, dtype=jnp.float32) / (NLON - 1)
    base = jnp.exp(jax.random.uniform(key, shape, jnp.float32, math.log(0.3), math.log(3.0)))
    return base * (1.0 + 2.0 * column)[:, None]


def draw_air_after(key, part):
    first_key, second_key = jax.random.split(jax.random.fold_in(key, 7))
    base = jnp.exp(jax.random.uniform(first_key, (LEV, NLON, NLAT), jnp.float32, math.log(0.5), math.log(2.0)))
    banded = jnp.clip(jax.random.normal(second_key, (LEV, 1, NLAT), jnp.float32), -2.5, 2.5)
    return base * jnp.exp(0.4 * banded)


def touch_ends(drawn, key, low, top_value):
    spot = [jax.random.randint(jax.random.fold_in(key, axis), (), 0, length) for axis, length in enumerate(drawn.shape)]
    main_axis = drawn.shape.index(max(drawn.shape))
    beside = spot[:main_axis] + [(spot[main_axis] + 1) % drawn.shape[main_axis]] + spot[main_axis + 1:]
    return drawn.at[tuple(spot)].set(low).at[tuple(beside)].set(top_value)


def block_scale(rng, shape, shards, low, largest):
    gain = 1.0
    for axis_at, blocks in shards:
        heights = jax.random.uniform(jax.random.fold_in(jax.random.fold_in(rng, 6), axis_at), (blocks,), jnp.float32, low / len(shards), largest / len(shards))
        gain = gain * jnp.repeat(jnp.exp(heights), shape[axis_at] // blocks).reshape((-1,) + (1,) * (len(shape) - 1 - axis_at))
    return gain


def setup_inputs(seed: int = 0, part: int = 0) -> dict:
    arg_keys = jax.random.split(jax.random.key(seed), 7)
    part_splits = jax.random.split(jax.random.fold_in(arg_keys[6], part), 7)
    return {
        "tracer": draw_tracer(jax.random.fold_in(jax.random.fold_in(arg_keys[6], part), 71), part),
        "offsets": touch_ends(jax.random.randint(arg_keys[1], (LEV, NLON, NLAT), -OFFMAX, OFFMAX + 1), jax.random.fold_in(arg_keys[1], 1), -OFFMAX, OFFMAX).astype(jnp.int32),
        "frac": jnp.clip(jax.random.uniform(arg_keys[2], (LEV, NLAT), jnp.float32, 0.02, 0.98), 0.02, 0.98),
        "air_before": jnp.clip(jnp.exp(math.log(2.0) - 1.3862944 * jax.random.uniform(arg_keys[3], (LEV, NLON, NLAT), jnp.float32) ** block_scale(arg_keys[3], (LEV, NLON, NLAT), ((1, 16),), -0.2, 0.2)), 0.5, 2.0),
        "air_after": draw_air_after(jax.random.fold_in(arg_keys[6], 71), part),
        "growth": jnp.clip(jnp.exp(jax.random.uniform(part_splits[5], (S,), jnp.float32, math.log(0.05), math.log(0.5))), 0.05, 0.5),
    }


def cubic_weights(fraction):
    first = -fraction * (1.0 - fraction) * (2.0 - fraction) / 6.0
    second = (1.0 + fraction) * (1.0 - fraction) * (2.0 - fraction) / 2.0
    third = (1.0 + fraction) * fraction * (2.0 - fraction) / 2.0
    fourth = -(1.0 + fraction) * fraction * (1.0 - fraction) / 6.0
    return first, second, third, fourth


def advect_species(species_field, offsets, weights):
    columns = lax.broadcasted_iota(jnp.int32, offsets.shape, 1)
    departure = (columns - offsets).astype(jnp.int32)
    stencil = []
    for offset_tap in range(4):
        position = ((departure - 1 + offset_tap) % NLON).astype(jnp.int32)
        stencil.append(jnp.take_along_axis(species_field, position, axis=1))
    cubic = weights[0] * stencil[0] + weights[1] * stencil[1]
    cubic = cubic + weights[2] * stencil[2] + weights[3] * stencil[3]
    lower_bound = jnp.minimum(stencil[1], stencil[2])
    upper_bound = jnp.maximum(stencil[1], stencil[2])
    return jnp.clip(cubic, lower_bound, upper_bound)


def reference(tracer, offsets, frac, air_before, air_after, growth):
    weights = tuple(item[:, None, :] for item in cubic_weights(frac))
    before_mass = jnp.sum(tracer * air_before[None], axis=(1, 2, 3))
    limited = lax.map(lambda field: advect_species(field, offsets, weights), tracer)
    after_mass = jnp.sum(limited * air_after[None], axis=(1, 2, 3))
    factor = before_mass * (1.0 + growth) / after_mass
    return limited * factor[:, None, None, None]
```

```python
import functools

import jax
import jax.numpy as jnp
from jax import lax
from jax.experimental import pallas as pl
from jax.experimental.pallas import tpu as pltpu
from jax.sharding import PartitionSpec as P

OFFMAX = 12
LOW = OFFMAX + 1
HIGH = OFFMAX + 2
LANES = 128
SUB = 8
SPLITS = 2
MESH = pl.DeviceIdType.MESH


def cubic_weights(fraction):
    first = -fraction * (1.0 - fraction) * (2.0 - fraction) / 6.0
    second = (1.0 + fraction) * (1.0 - fraction) * (2.0 - fraction) / 2.0
    third = (1.0 + fraction) * fraction * (2.0 - fraction) / 2.0
    fourth = -(1.0 + fraction) * fraction * (1.0 - fraction) / 6.0
    return (first, second, third, fourth)


def transport_kernel(
    count,
    growth_ref,
    tracer_hbm,
    offsets_hbm,
    frac_ref,
    before_hbm,
    after_hbm,
    limited_hbm,
    factor_ref,
    tracer,
    limited,
    offsets,
    air_before,
    air_after,
    send_low,
    send_high,
    recv_low,
    recv_high,
    padded,
    sums,
    mine,
    masses,
    load_sem,
    air_sem,
    store_sem,
    send_sem,
    recv_sem,
    mass_send,
    mass_recv,
):
    species, levels, rows, lats = tracer.shape
    chunks = levels * SPLITS
    blocks = lats // LANES // SPLITS
    width = blocks * LANES
    me = lax.axis_index("lon")
    right = lax.rem(me + 1, count)
    left = lax.rem(me + count - 1, count)
    span = rows + 2 * OFFMAX

    def load(chunk):
        level = chunk // SPLITS
        lanes = pl.ds(pl.multiple_of(lax.rem(chunk, SPLITS) * width, width), width)
        return pltpu.make_async_copy(
            tracer_hbm.at[:, level, :, lanes], tracer.at[:, level, :, lanes], load_sem.at[chunk]
        )

    def store(chunk):
        level = chunk // SPLITS
        lanes = pl.ds(pl.multiple_of(lax.rem(chunk, SPLITS) * width, width), width)
        return pltpu.make_async_copy(
            limited.at[:, level, :, lanes], limited_hbm.at[:, level, :, lanes], store_sem.at[chunk]
        )

    airs = [
        pltpu.make_async_copy(before_hbm, air_before, air_sem.at[0]),
        pltpu.make_async_copy(offsets_hbm, offsets, air_sem.at[1]),
        pltpu.make_async_copy(after_hbm, air_after, air_sem.at[2]),
    ]

    def forward(chunk):
        return pltpu.make_async_remote_copy(
            src_ref=send_low.at[chunk],
            dst_ref=recv_low.at[chunk],
            send_sem=send_sem.at[0, chunk],
            recv_sem=recv_sem.at[0, chunk],
            device_id={"lon": right},
            device_id_type=MESH,
        )

    def backward(chunk):
        return pltpu.make_async_remote_copy(
            src_ref=send_high.at[chunk],
            dst_ref=recv_high.at[chunk],
            send_sem=send_sem.at[1, chunk],
            recv_sem=recv_sem.at[1, chunk],
            device_id={"lon": left},
            device_id_type=MESH,
        )

    barrier = pltpu.get_barrier_semaphore()

    @pl.loop(1, count)
    def _(step):
        peer = lax.rem(me + step, count)
        pl.semaphore_signal(barrier, inc=1, device_id={"lon": peer}, device_id_type=MESH)

    @pl.loop(0, chunks)
    def _(chunk):
        load(chunk).start()

    for copy in airs:
        copy.start()
    pl.semaphore_wait(barrier, count - 1)

    @pl.loop(0, chunks)
    def _(chunk):
        load(chunk).wait()
        level = chunk // SPLITS

        @pl.loop(0, blocks)
        def _(block):
            at = pl.multiple_of((lax.rem(chunk, SPLITS) * blocks + block) * LANES, LANES)
            lanes = pl.ds(at, LANES)
            for s in range(species):
                send_low[chunk, block, s * LOW : (s + 1) * LOW, :] = tracer[
                    s, level, rows - LOW : rows, lanes
                ]
                send_high[chunk, block, s * HIGH : (s + 1) * HIGH, :] = tracer[
                    s, level, 0:HIGH, lanes
                ]

        forward(chunk).start()
        backward(chunk).start()

    sums[...] = jnp.zeros_like(sums)
    for copy in airs:
        copy.wait()

    @pl.loop(0, chunks)
    def _(chunk):
        level = chunk // SPLITS

        @pl.loop(0, blocks)
        def _(block):
            at = pl.multiple_of((lax.rem(chunk, SPLITS) * blocks + block) * LANES, LANES)
            lanes = pl.ds(at, LANES)
            air = air_before[level, :, lanes]
            for s in range(species):
                mass = tracer[s, level, :, lanes] * air
                sums[0, s] += jnp.sum(mass.reshape(rows // SUB, SUB, LANES), axis=0)

    @pl.loop(0, chunks)
    def _(chunk):
        level = chunk // SPLITS
        forward(chunk).wait_recv()
        backward(chunk).wait_recv()

        @pl.loop(0, blocks)
        def _(block):
            at = pl.multiple_of((lax.rem(chunk, SPLITS) * blocks + block) * LANES, LANES)
            lanes = pl.ds(at, LANES)
            fraction = frac_ref[:, lanes]
            pick = lax.broadcasted_iota(jnp.int32, fraction.shape, 0) == level
            fraction = jnp.sum(jnp.where(pick, fraction, 0.0), axis=0, keepdims=True)
            weights = cubic_weights(fraction)
            weights = [jnp.broadcast_to(item, (span, LANES)) for item in weights]
            row = lax.broadcasted_iota(jnp.int32, (SUB, LANES), 0)
            picks = []
            for d in range(rows // SUB):
                local = row - offsets[level, d * SUB : (d + 1) * SUB, lanes] + OFFMAX
                picks.append((lax.bitwise_and(local, SUB - 1), lax.shift_right_logical(local, 3)))
            for s in range(species):
                padded[s, 0:LOW, :] = recv_low[chunk, block, s * LOW : (s + 1) * LOW, :]
                padded[s, LOW : LOW + rows, :] = tracer[s, level, :, lanes]
                padded[s, LOW + rows : LOW + rows + HIGH, :] = recv_high[
                    chunk, block, s * HIGH : (s + 1) * HIGH, :
                ]
                taps = [padded[s, tap : tap + span, :] for tap in range(4)]
                cubic = weights[0] * taps[0] + weights[1] * taps[1]
                cubic = cubic + weights[2] * taps[2] + weights[3] * taps[3]
                lower = jnp.minimum(taps[1], taps[2])
                upper = jnp.maximum(taps[1], taps[2])
                values = jnp.minimum(jnp.maximum(cubic, lower), upper)
                total = sums[1, s]
                for d in range(rows // SUB):
                    spot, which = picks[d]
                    result = None
                    for h in range(4):
                        source = values[(d + h) * SUB : (d + h + 1) * SUB]
                        got = jnp.take_along_axis(
                            source, spot, axis=0, mode="promise_in_bounds"
                        )
                        result = got if result is None else jnp.where(which == h, got, result)
                    limited[s, level, d * SUB : (d + 1) * SUB, lanes] = result
                    total = total + result * air_after[level, d * SUB : (d + 1) * SUB, lanes]
                sums[1, s] = total

        store(chunk).start()

    lane = lax.broadcasted_iota(jnp.int32, (1, LANES), 1)
    line = jnp.zeros((1, LANES), jnp.float32)
    for which in range(2):
        for s in range(species):
            value = jnp.sum(sums[which, s], keepdims=True)
            line = jnp.where(lane == which * species + s, value, line)
    mine[...] = line
    masses[me] = line

    def share(step):
        return pltpu.make_async_remote_copy(
            src_ref=mine,
            dst_ref=masses.at[me],
            send_sem=mass_send.at[step],
            recv_sem=mass_recv.at[me],
            device_id={"lon": lax.rem(me + step, count)},
            device_id_type=MESH,
        )

    def arrive(step):
        source = lax.rem(me + count - step, count)
        return pltpu.make_async_remote_copy(
            src_ref=mine,
            dst_ref=masses.at[source],
            send_sem=mass_send.at[step],
            recv_sem=mass_recv.at[source],
            device_id={"lon": source},
            device_id_type=MESH,
        )

    @pl.loop(1, count)
    def _(step):
        share(step).start()

    @pl.loop(0, chunks)
    def _(chunk):
        forward(chunk).wait_send()
        backward(chunk).wait_send()
        store(chunk).wait()

    @pl.loop(1, count)
    def _(step):
        arrive(step).wait_recv()

    total = masses[0]
    for j in range(1, count):
        total = total + masses[j]
    grow = jnp.zeros((1, LANES), jnp.float32)
    for s in range(species):
        grow = jnp.where(lane == s, growth_ref[s], grow)
    later = pltpu.roll(total, LANES - species, axis=1)
    later = jnp.where(lane < species, later, 1.0)
    factor_ref[...] = total * (1.0 + grow) / later

    @pl.loop(1, count)
    def _(step):
        share(step).wait_send()


def on_device(tracer, offsets, frac, air_before, air_after, growth):
    species, levels, rows, lats = tracer.shape
    count = lax.axis_size("lon")
    chunks = levels * SPLITS
    blocks = lats // LANES // SPLITS
    any_spec = pl.BlockSpec(memory_space=pl.ANY)
    vmem_spec = pl.BlockSpec(memory_space=pltpu.VMEM)
    f32 = jnp.float32
    limited, factor = pl.pallas_call(
        functools.partial(transport_kernel, count),
        out_shape=(
            jax.ShapeDtypeStruct(tracer.shape, f32),
            jax.ShapeDtypeStruct((1, LANES), f32),
        ),
        in_specs=[
            pl.BlockSpec(memory_space=pltpu.SMEM),
            any_spec,
            any_spec,
            vmem_spec,
            any_spec,
            any_spec,
        ],
        out_specs=(any_spec, vmem_spec),
        scratch_shapes=[
            pltpu.VMEM(tracer.shape, f32),
            pltpu.VMEM(tracer.shape, f32),
            pltpu.VMEM(offsets.shape, jnp.int32),
            pltpu.VMEM(offsets.shape, f32),
            pltpu.VMEM(offsets.shape, f32),
            pltpu.VMEM((chunks, blocks, species * LOW, LANES), f32),
            pltpu.VMEM((chunks, blocks, species * HIGH, LANES), f32),
            pltpu.VMEM((chunks, blocks, species * LOW, LANES), f32),
            pltpu.VMEM((chunks, blocks, species * HIGH, LANES), f32),
            pltpu.VMEM((species, rows + 4 * SUB, LANES), f32),
            pltpu.VMEM((2, species, SUB, LANES), f32),
            pltpu.VMEM((1, LANES), f32),
            pltpu.VMEM((count, 1, LANES), f32),
            pltpu.SemaphoreType.DMA((chunks,)),
            pltpu.SemaphoreType.DMA((3,)),
            pltpu.SemaphoreType.DMA((chunks,)),
            pltpu.SemaphoreType.DMA((2, chunks)),
            pltpu.SemaphoreType.DMA((2, chunks)),
            pltpu.SemaphoreType.DMA((count,)),
            pltpu.SemaphoreType.DMA((count,)),
        ],
        compiler_params=pltpu.CompilerParams(
            collective_id=0, has_side_effects=True, vmem_limit_bytes=40 * 1024 * 1024
        ),
        name="transport",
    )(growth, tracer, offsets, frac, air_before, air_after)
    return limited * factor[0, :species][:, None, None, None]


def solution(mesh):
    placed = (
        P("scen", None, "lon", None),
        P(None, "lon", None),
        P(),
        P(None, "lon", None),
        P(None, "lon", None),
        P("scen"),
    )
    return jax.shard_map(
        on_device,
        mesh=mesh,
        in_specs=placed,
        out_specs=P("scen", None, "lon", None),
        check_vma=False,
    )
```

```python
import functools

import jax
import jax.numpy as jnp
from jax import lax
from jax.experimental import pallas as pl
from jax.experimental.pallas import tpu as pltpu
from jax.sharding import PartitionSpec as P

OFFMAX = 12
LOW = OFFMAX + 1
HIGH = OFFMAX + 2
LANES = 128
SUB = 8
SPLITS = 4
MESH = pl.DeviceIdType.MESH


def cubic_weights(fraction):
    first = -fraction * (1.0 - fraction) * (2.0 - fraction) / 6.0
    second = (1.0 + fraction) * (1.0 - fraction) * (2.0 - fraction) / 2.0
    third = (1.0 + fraction) * fraction * (2.0 - fraction) / 2.0
    fourth = -(1.0 + fraction) * fraction * (1.0 - fraction) / 6.0
    return (first, second, third, fourth)


def transport_kernel(
    count,
    tracer_hbm,
    offsets_hbm,
    frac_hbm,
    before_hbm,
    after_hbm,
    growth_hbm,
    limited_hbm,
    factor_ref,
    tracer,
    limited,
    offsets,
    air_before,
    air_after,
    frac_ref,
    growth_ref,
    send_low,
    send_high,
    recv_low,
    recv_high,
    padded,
    sums,
    mine,
    masses,
    load_sem,
    air_sem,
    store_sem,
    send_sem,
    recv_sem,
    mass_send,
    mass_recv,
):
    species, levels, rows, lats = tracer.shape
    chunks = levels * SPLITS
    blocks = lats // LANES // SPLITS
    width = blocks * LANES
    me = lax.axis_index("lon")
    right = lax.rem(me + 1, count)
    left = lax.rem(me + count - 1, count)
    span = rows + 2 * OFFMAX

    def load(chunk):
        level = chunk // SPLITS
        lanes = pl.ds(pl.multiple_of(lax.rem(chunk, SPLITS) * width, width), width)
        return pltpu.make_async_copy(
            tracer_hbm.at[:, level, :, lanes], tracer.at[:, level, :, lanes], load_sem.at[chunk]
        )

    def store(chunk):
        level = chunk // SPLITS
        lanes = pl.ds(pl.multiple_of(lax.rem(chunk, SPLITS) * width, width), width)
        return pltpu.make_async_copy(
            limited.at[:, level, :, lanes], limited_hbm.at[:, level, :, lanes], store_sem.at[chunk]
        )

    airs = [
        pltpu.make_async_copy(before_hbm, air_before, air_sem.at[0]),
        pltpu.make_async_copy(offsets_hbm, offsets, air_sem.at[1]),
        pltpu.make_async_copy(after_hbm, air_after, air_sem.at[2]),
        pltpu.make_async_copy(frac_hbm, frac_ref, air_sem.at[3]),
        pltpu.make_async_copy(growth_hbm, growth_ref, air_sem.at[4]),
    ]

    def forward(chunk):
        return pltpu.make_async_remote_copy(
            src_ref=send_low.at[chunk],
            dst_ref=recv_low.at[chunk],
            send_sem=send_sem.at[0, chunk],
            recv_sem=recv_sem.at[0, chunk],
            device_id={"lon": right},
            device_id_type=MESH,
        )

    def backward(chunk):
        return pltpu.make_async_remote_copy(
            src_ref=send_high.at[chunk],
            dst_ref=recv_high.at[chunk],
            send_sem=send_sem.at[1, chunk],
            recv_sem=recv_sem.at[1, chunk],
            device_id={"lon": left},
            device_id_type=MESH,
        )

    def pack(chunk):
        load(chunk).wait()
        level = chunk // SPLITS

        @pl.loop(0, blocks)
        def _(block):
            at = pl.multiple_of((lax.rem(chunk, SPLITS) * blocks + block) * LANES, LANES)
            lanes = pl.ds(at, LANES)
            for s in range(species):
                send_low[chunk, block, s * LOW : (s + 1) * LOW, :] = tracer[
                    s, level, rows - LOW : rows, lanes
                ]
                send_high[chunk, block, s * HIGH : (s + 1) * HIGH, :] = tracer[
                    s, level, 0:HIGH, lanes
                ]

    load(0).start()
    barrier = pltpu.get_barrier_semaphore()

    @pl.loop(1, count)
    def _(step):
        peer = lax.rem(me + step, count)
        pl.semaphore_signal(barrier, inc=1, device_id={"lon": peer}, device_id_type=MESH)

    @pl.loop(1, chunks)
    def _(chunk):
        load(chunk).start()

    for copy in airs:
        copy.start()
    pack(0)
    pl.semaphore_wait(barrier, count - 1)
    forward(0).start()
    backward(0).start()

    @pl.loop(1, chunks)
    def _(chunk):
        pack(chunk)
        forward(chunk).start()
        backward(chunk).start()

    sums[...] = jnp.zeros_like(sums)
    for copy in airs:
        copy.wait()

    @pl.loop(0, chunks)
    def _(chunk):
        level = chunk // SPLITS

        @pl.loop(0, blocks)
        def _(block):
            at = pl.multiple_of((lax.rem(chunk, SPLITS) * blocks + block) * LANES, LANES)
            lanes = pl.ds(at, LANES)
            air = air_before[level, :, lanes]
            for s in range(species):
                mass = tracer[s, level, :, lanes] * air
                sums[0, s] += jnp.sum(mass.reshape(rows // SUB, SUB, LANES), axis=0)

    lane = lax.broadcasted_iota(jnp.int32, (1, LANES), 1)

    def gathered(which, line):
        for s in range(species):
            value = jnp.sum(sums[which, s], keepdims=True)
            line = jnp.where(lane == which * species + s, value, line)
        return line

    mine[...] = gathered(0, jnp.zeros((1, LANES), jnp.float32))

    @pl.loop(0, chunks)
    def _(chunk):
        level = chunk // SPLITS
        forward(chunk).wait_recv()
        backward(chunk).wait_recv()

        @pl.loop(0, blocks)
        def _(block):
            at = pl.multiple_of((lax.rem(chunk, SPLITS) * blocks + block) * LANES, LANES)
            lanes = pl.ds(at, LANES)
            fraction = frac_ref[:, lanes]
            pick = lax.broadcasted_iota(jnp.int32, fraction.shape, 0) == level
            fraction = jnp.sum(jnp.where(pick, fraction, 0.0), axis=0, keepdims=True)
            weights = cubic_weights(fraction)
            weights = [jnp.broadcast_to(item, (span, LANES)) for item in weights]
            row = lax.broadcasted_iota(jnp.int32, (SUB, LANES), 0)
            picks = []
            for d in range(rows // SUB):
                local = row - offsets[level, d * SUB : (d + 1) * SUB, lanes] + OFFMAX
                picks.append((lax.bitwise_and(local, SUB - 1), lax.shift_right_logical(local, 3)))
            for s in range(species):
                padded[s, 0:LOW, :] = recv_low[chunk, block, s * LOW : (s + 1) * LOW, :]
                padded[s, LOW : LOW + rows, :] = tracer[s, level, :, lanes]
                padded[s, LOW + rows : LOW + rows + HIGH, :] = recv_high[
                    chunk, block, s * HIGH : (s + 1) * HIGH, :
                ]
                taps = [padded[s, tap : tap + span, :] for tap in range(4)]
                cubic = weights[0] * taps[0] + weights[1] * taps[1]
                cubic = cubic + weights[2] * taps[2] + weights[3] * taps[3]
                lower = jnp.minimum(taps[1], taps[2])
                upper = jnp.maximum(taps[1], taps[2])
                values = jnp.minimum(jnp.maximum(cubic, lower), upper)
                total = sums[1, s]
                for d in range(rows // SUB):
                    spot, which = picks[d]
                    result = None
                    for h in range(4):
                        source = values[(d + h) * SUB : (d + h + 1) * SUB]
                        got = jnp.take_along_axis(
                            source, spot, axis=0, mode="promise_in_bounds"
                        )
                        result = got if result is None else jnp.where(which == h, got, result)
                    limited[s, level, d * SUB : (d + 1) * SUB, lanes] = result
                    total = total + result * air_after[level, d * SUB : (d + 1) * SUB, lanes]
                sums[1, s] = total

        store(chunk).start()

    line = gathered(1, mine[...])
    mine[...] = line
    masses[me] = line

    def share(step):
        return pltpu.make_async_remote_copy(
            src_ref=mine,
            dst_ref=masses.at[me],
            send_sem=mass_send.at[step],
            recv_sem=mass_recv.at[me],
            device_id={"lon": lax.rem(me + step, count)},
            device_id_type=MESH,
        )

    def arrive(step):
        source = lax.rem(me + count - step, count)
        return pltpu.make_async_remote_copy(
            src_ref=mine,
            dst_ref=masses.at[source],
            send_sem=mass_send.at[step],
            recv_sem=mass_recv.at[source],
            device_id={"lon": source},
            device_id_type=MESH,
        )

    @pl.loop(1, count)
    def _(step):
        share(step).start()

    @pl.loop(0, chunks)
    def _(chunk):
        forward(chunk).wait_send()
        backward(chunk).wait_send()
        store(chunk).wait()

    @pl.loop(1, count)
    def _(step):
        arrive(step).wait_recv()

    total = masses[0]
    for j in range(1, count):
        total = total + masses[j]
    grow = jnp.zeros((1, LANES), jnp.float32)
    for s in range(species):
        grow = jnp.where(lane == s, growth_ref[s], grow)
    later = pltpu.roll(total, LANES - species, axis=1)
    later = jnp.where(lane < species, later, 1.0)
    factor_ref[...] = total * (1.0 + grow) / later

    @pl.loop(1, count)
    def _(step):
        share(step).wait_send()


def on_device(tracer, offsets, frac, air_before, air_after, growth):
    species, levels, rows, lats = tracer.shape
    count = lax.axis_size("lon")
    chunks = levels * SPLITS
    blocks = lats // LANES // SPLITS
    any_spec = pl.BlockSpec(memory_space=pl.ANY)
    hbm_spec = pl.BlockSpec(memory_space=pltpu.HBM)
    vmem_spec = pl.BlockSpec(memory_space=pltpu.VMEM)
    f32 = jnp.float32
    limited, factor = pl.pallas_call(
        functools.partial(transport_kernel, count),
        out_shape=(
            jax.ShapeDtypeStruct(tracer.shape, f32),
            jax.ShapeDtypeStruct((1, LANES), f32),
        ),
        in_specs=[hbm_spec] * 6,
        out_specs=(any_spec, vmem_spec),
        scratch_shapes=[
            pltpu.VMEM(tracer.shape, f32),
            pltpu.VMEM(tracer.shape, f32),
            pltpu.VMEM(offsets.shape, jnp.int32),
            pltpu.VMEM(offsets.shape, f32),
            pltpu.VMEM(offsets.shape, f32),
            pltpu.VMEM(frac.shape, f32),
            pltpu.SMEM(growth.shape, f32),
            pltpu.VMEM((chunks, blocks, species * LOW, LANES), f32),
            pltpu.VMEM((chunks, blocks, species * HIGH, LANES), f32),
            pltpu.VMEM((chunks, blocks, species * LOW, LANES), f32),
            pltpu.VMEM((chunks, blocks, species * HIGH, LANES), f32),
            pltpu.VMEM((species, rows + 4 * SUB, LANES), f32),
            pltpu.VMEM((2, species, SUB, LANES), f32),
            pltpu.VMEM((1, LANES), f32),
            pltpu.VMEM((count, 1, LANES), f32),
            pltpu.SemaphoreType.DMA((chunks,)),
            pltpu.SemaphoreType.DMA((5,)),
            pltpu.SemaphoreType.DMA((chunks,)),
            pltpu.SemaphoreType.DMA((2, chunks)),
            pltpu.SemaphoreType.DMA((2, chunks)),
            pltpu.SemaphoreType.DMA((count,)),
            pltpu.SemaphoreType.DMA((count,)),
        ],
        compiler_params=pltpu.CompilerParams(
            collective_id=0, has_side_effects=True, vmem_limit_bytes=58 * 1024 * 1024
        ),
        name="transport",
    )(tracer, offsets, frac, air_before, air_after, growth)
    return limited * factor[0, :species][:, None, None, None]


def solution(mesh):
    placed = (
        P("scen", None, "lon", None),
        P(None, "lon", None),
        P(),
        P(None, "lon", None),
        P(None, "lon", None),
        P("scen"),
    )
    return jax.shard_map(
        on_device,
        mesh=mesh,
        in_specs=placed,
        out_specs=P("scen", None, "lon", None),
        check_vma=False,
    )
```

```python
import functools

import jax
import jax.numpy as jnp
from jax import lax
from jax.experimental import pallas as pl
from jax.experimental.pallas import tpu as pltpu
from jax.sharding import PartitionSpec as P

OFFMAX = 12
LOW = OFFMAX + 1
HIGH = OFFMAX + 2
LANES = 128
SUB = 8
SPLITS = 4
MESH = pl.DeviceIdType.MESH


def cubic_weights(fraction):
    first = -fraction * (1.0 - fraction) * (2.0 - fraction) / 6.0
    second = (1.0 + fraction) * (1.0 - fraction) * (2.0 - fraction) / 2.0
    third = (1.0 + fraction) * fraction * (2.0 - fraction) / 2.0
    fourth = -(1.0 + fraction) * fraction * (1.0 - fraction) / 6.0
    return (first, second, third, fourth)


def transport_kernel(
    count,
    tracer_hbm,
    offsets_hbm,
    frac_hbm,
    before_hbm,
    after_hbm,
    growth_hbm,
    limited_hbm,
    factor_ref,
    tracer,
    limited,
    offsets,
    air_before,
    air_after,
    frac_ref,
    growth_ref,
    send_low,
    send_high,
    recv_low,
    recv_high,
    padded,
    sums,
    mine,
    masses,
    load_sem,
    air_sem,
    store_sem,
    send_sem,
    recv_sem,
    mass_send,
    mass_recv,
):
    species, levels, rows, lats = tracer.shape
    chunks = levels * SPLITS
    blocks = lats // LANES // SPLITS
    width = blocks * LANES
    me = lax.axis_index("lon")
    right = lax.rem(me + 1, count)
    left = lax.rem(me + count - 1, count)
    span = rows + 2 * OFFMAX

    def load(chunk):
        level = chunk // SPLITS
        lanes = pl.ds(pl.multiple_of(lax.rem(chunk, SPLITS) * width, width), width)
        return pltpu.make_async_copy(
            tracer_hbm.at[:, level, :, lanes], tracer.at[:, level, :, lanes], load_sem.at[chunk]
        )

    def store(chunk):
        level = chunk // SPLITS
        lanes = pl.ds(pl.multiple_of(lax.rem(chunk, SPLITS) * width, width), width)
        return pltpu.make_async_copy(
            limited.at[:, level, :, lanes], limited_hbm.at[:, level, :, lanes], store_sem.at[chunk]
        )

    airs = [
        pltpu.make_async_copy(before_hbm, air_before, air_sem.at[0]),
        pltpu.make_async_copy(offsets_hbm, offsets, air_sem.at[1]),
        pltpu.make_async_copy(after_hbm, air_after, air_sem.at[2]),
        pltpu.make_async_copy(frac_hbm, frac_ref, air_sem.at[3]),
        pltpu.make_async_copy(growth_hbm, growth_ref, air_sem.at[4]),
    ]

    def forward(chunk):
        return pltpu.make_async_remote_copy(
            src_ref=send_low.at[chunk],
            dst_ref=recv_low.at[chunk],
            send_sem=send_sem.at[0, chunk],
            recv_sem=recv_sem.at[0, chunk],
            device_id={"lon": right},
            device_id_type=MESH,
        )

    def backward(chunk):
        return pltpu.make_async_remote_copy(
            src_ref=send_high.at[chunk],
            dst_ref=recv_high.at[chunk],
            send_sem=send_sem.at[1, chunk],
            recv_sem=recv_sem.at[1, chunk],
            device_id={"lon": left},
            device_id_type=MESH,
        )

    def pack(chunk):
        load(chunk).wait()
        level = chunk // SPLITS

        @pl.loop(0, blocks)
        def _(block):
            at = pl.multiple_of((lax.rem(chunk, SPLITS) * blocks + block) * LANES, LANES)
            lanes = pl.ds(at, LANES)
            for s in range(species):
                send_low[chunk, block, s * LOW : (s + 1) * LOW, :] = tracer[
                    s, level, rows - LOW : rows, lanes
                ]
                send_high[chunk, block, s * HIGH : (s + 1) * HIGH, :] = tracer[
                    s, level, 0:HIGH, lanes
                ]

    load(0).start()
    barrier = pltpu.get_barrier_semaphore()

    @pl.loop(1, count)
    def _(step):
        peer = lax.rem(me + step, count)
        pl.semaphore_signal(barrier, inc=1, device_id={"lon": peer}, device_id_type=MESH)

    @pl.loop(1, chunks)
    def _(chunk):
        load(chunk).start()

    for copy in airs:
        copy.start()
    pack(0)
    pl.semaphore_wait(barrier, count - 1)
    forward(0).start()
    backward(0).start()

    @pl.loop(1, chunks)
    def _(chunk):
        pack(chunk)
        forward(chunk).start()
        backward(chunk).start()

    sums[...] = jnp.zeros_like(sums)
    for copy in airs:
        copy.wait()

    @pl.loop(0, chunks)
    def _(chunk):
        level = chunk // SPLITS

        @pl.loop(0, blocks)
        def _(block):
            at = pl.multiple_of((lax.rem(chunk, SPLITS) * blocks + block) * LANES, LANES)
            lanes = pl.ds(at, LANES)
            air = air_before[level, :, lanes]
            for s in range(species):
                mass = tracer[s, level, :, lanes] * air
                sums[0, s] += jnp.sum(mass.reshape(rows // SUB, SUB, LANES), axis=0)

    lane = lax.broadcasted_iota(jnp.int32, (1, LANES), 1)

    def gathered(which, line):
        for s in range(species):
            value = jnp.sum(sums[which, s], keepdims=True)
            line = jnp.where(lane == which * species + s, value, line)
        return line

    mine[...] = gathered(0, jnp.zeros((1, LANES), jnp.float32))

    @pl.loop(0, chunks)
    def _(chunk):
        level = chunk // SPLITS
        forward(chunk).wait_recv()
        backward(chunk).wait_recv()

        @pl.loop(0, blocks)
        def _(block):
            at = pl.multiple_of((lax.rem(chunk, SPLITS) * blocks + block) * LANES, LANES)
            lanes = pl.ds(at, LANES)
            fraction = frac_ref[:, lanes]
            pick = lax.broadcasted_iota(jnp.int32, fraction.shape, 0) == level
            fraction = jnp.sum(jnp.where(pick, fraction, 0.0), axis=0, keepdims=True)
            weights = cubic_weights(fraction)
            weights = [jnp.broadcast_to(item, (span, LANES)) for item in weights]
            row = lax.broadcasted_iota(jnp.int32, (SUB, LANES), 0)
            picks = []
            for d in range(rows // SUB):
                local = row - offsets[level, d * SUB : (d + 1) * SUB, lanes] + OFFMAX
                picks.append((lax.bitwise_and(local, SUB - 1), lax.shift_right_logical(local, 3)))
            for s in range(species):
                padded[s, 0:LOW, :] = recv_low[chunk, block, s * LOW : (s + 1) * LOW, :]
                padded[s, LOW : LOW + rows, :] = tracer[s, level, :, lanes]
                padded[s, LOW + rows : LOW + rows + HIGH, :] = recv_high[
                    chunk, block, s * HIGH : (s + 1) * HIGH, :
                ]
                taps = [padded[s, tap : tap + span, :] for tap in range(4)]
                cubic = weights[0] * taps[0] + weights[1] * taps[1]
                cubic = cubic + weights[2] * taps[2] + weights[3] * taps[3]
                lower = jnp.minimum(taps[1], taps[2])
                upper = jnp.maximum(taps[1], taps[2])
                values = jnp.minimum(jnp.maximum(cubic, lower), upper)
                total = sums[1, s]
                for d in range(rows // SUB):
                    spot, which = picks[d]
                    result = None
                    for h in range(4):
                        source = values[(d + h) * SUB : (d + h + 1) * SUB]
                        got = jnp.take_along_axis(
                            source, spot, axis=0, mode="promise_in_bounds"
                        )
                        result = got if result is None else jnp.where(which == h, got, result)
                    limited[s, level, d * SUB : (d + 1) * SUB, lanes] = result
                    total = total + result * air_after[level, d * SUB : (d + 1) * SUB, lanes]
                sums[1, s] = total

        store(chunk).start()

    line = gathered(1, mine[...])
    mine[...] = line
    masses[me] = line

    def share(step):
        return pltpu.make_async_remote_copy(
            src_ref=mine,
            dst_ref=masses.at[me],
            send_sem=mass_send.at[step],
            recv_sem=mass_recv.at[me],
            device_id={"lon": lax.rem(me + step, count)},
            device_id_type=MESH,
        )

    def arrive(step):
        source = lax.rem(me + count - step, count)
        return pltpu.make_async_remote_copy(
            src_ref=mine,
            dst_ref=masses.at[source],
            send_sem=mass_send.at[step],
            recv_sem=mass_recv.at[source],
            device_id={"lon": source},
            device_id_type=MESH,
        )

    @pl.loop(1, count)
    def _(step):
        share(step).start()

    @pl.loop(0, chunks)
    def _(chunk):
        forward(chunk).wait_send()
        backward(chunk).wait_send()
        store(chunk).wait()

    @pl.loop(1, count)
    def _(step):
        arrive(step).wait_recv()

    total = masses[0]
    for j in range(1, count):
        total = total + masses[j]
    grow = jnp.zeros((1, LANES), jnp.float32)
    for s in range(species):
        grow = jnp.where(lane == s, growth_ref[s], grow)
    later = pltpu.roll(total, LANES - species, axis=1)
    later = jnp.where(lane < species, later, 1.0)
    factor_ref[...] = total * (1.0 + grow) / later

    @pl.loop(1, count)
    def _(step):
        share(step).wait_send()


def scale_kernel(
    limited_hbm, factor_hbm, scaled_hbm, values, factor, read_sem, write_sem, factor_sem
):
    species, levels = values.shape[:2]
    ready = pltpu.make_async_copy(factor_hbm, factor, factor_sem)
    ready.start()

    def read(s, level):
        return pltpu.make_async_copy(
            limited_hbm.at[s, level], values.at[s, level], read_sem.at[s, level]
        )

    def write(s, level):
        return pltpu.make_async_copy(
            values.at[s, level], scaled_hbm.at[s, level], write_sem.at[s, level]
        )

    @pl.loop(0, species)
    def _(s):
        for level in range(levels):
            read(s, level).start()

    ready.wait()
    lane = lax.broadcasted_iota(jnp.int32, (1, LANES), 1)

    @pl.loop(0, species)
    def _(s):
        scale = jnp.sum(jnp.where(lane == s, factor[...], 0.0), axis=1, keepdims=True)
        for level in range(levels):
            read(s, level).wait()
            values[s, level] = values[s, level] * scale
            write(s, level).start()

    @pl.loop(0, species)
    def _(s):
        for level in range(levels):
            write(s, level).wait()


def on_device(tracer, offsets, frac, air_before, air_after, growth):
    species, levels, rows, lats = tracer.shape
    count = lax.axis_size("lon")
    chunks = levels * SPLITS
    blocks = lats // LANES // SPLITS
    any_spec = pl.BlockSpec(memory_space=pl.ANY)
    hbm_spec = pl.BlockSpec(memory_space=pltpu.HBM)
    vmem_spec = pl.BlockSpec(memory_space=pltpu.VMEM)
    f32 = jnp.float32
    limited, factor = pl.pallas_call(
        functools.partial(transport_kernel, count),
        out_shape=(
            jax.ShapeDtypeStruct(tracer.shape, f32),
            jax.ShapeDtypeStruct((1, LANES), f32),
        ),
        in_specs=[hbm_spec] * 6,
        out_specs=(any_spec, vmem_spec),
        scratch_shapes=[
            pltpu.VMEM(tracer.shape, f32),
            pltpu.VMEM(tracer.shape, f32),
            pltpu.VMEM(offsets.shape, jnp.int32),
            pltpu.VMEM(offsets.shape, f32),
            pltpu.VMEM(offsets.shape, f32),
            pltpu.VMEM(frac.shape, f32),
            pltpu.SMEM(growth.shape, f32),
            pltpu.VMEM((chunks, blocks, species * LOW, LANES), f32),
            pltpu.VMEM((chunks, blocks, species * HIGH, LANES), f32),
            pltpu.VMEM((chunks, blocks, species * LOW, LANES), f32),
            pltpu.VMEM((chunks, blocks, species * HIGH, LANES), f32),
            pltpu.VMEM((species, rows + 4 * SUB, LANES), f32),
            pltpu.VMEM((2, species, SUB, LANES), f32),
            pltpu.VMEM((1, LANES), f32),
            pltpu.VMEM((count, 1, LANES), f32),
            pltpu.SemaphoreType.DMA((chunks,)),
            pltpu.SemaphoreType.DMA((5,)),
            pltpu.SemaphoreType.DMA((chunks,)),
            pltpu.SemaphoreType.DMA((2, chunks)),
            pltpu.SemaphoreType.DMA((2, chunks)),
            pltpu.SemaphoreType.DMA((count,)),
            pltpu.SemaphoreType.DMA((count,)),
        ],
        compiler_params=pltpu.CompilerParams(
            collective_id=0, has_side_effects=True, vmem_limit_bytes=58 * 1024 * 1024
        ),
        name="transport",
    )(tracer, offsets, frac, air_before, air_after, growth)
    return pl.pallas_call(
        scale_kernel,
        out_shape=jax.ShapeDtypeStruct(tracer.shape, f32),
        in_specs=[any_spec, any_spec],
        out_specs=any_spec,
        scratch_shapes=[
            pltpu.VMEM(tracer.shape, f32),
            pltpu.VMEM((1, LANES), f32),
            pltpu.SemaphoreType.DMA((species, levels)),
            pltpu.SemaphoreType.DMA((species, levels)),
            pltpu.SemaphoreType.DMA,
        ],
        compiler_params=pltpu.CompilerParams(vmem_limit_bytes=58 * 1024 * 1024),
        name="scale",
    )(limited, factor)


def solution(mesh):
    placed = (
        P("scen", None, "lon", None),
        P(None, "lon", None),
        P(),
        P(None, "lon", None),
        P(None, "lon", None),
        P("scen"),
    )
    return jax.shard_map(
        on_device,
        mesh=mesh,
        in_specs=placed,
        out_specs=P("scen", None, "lon", None),
        check_vma=False,
    )
```
